32 devices in a mesh: vocab: 8 (over z, y), layer: 4 (over x, core).
Axes of the slice: x: 2, y: 2, z: 4, core: 2. Of those that a mesh axis runs over, the one named last changes fastest.
Arguments:
- residual: bfloat16 [1024, 8192], P('layer', 'vocab'), may hold values from -40 to 40
- gain: bfloat16 [1, 8192], P(None, 'vocab'), may hold values from 0.25 to 1.75
- unembed: bfloat16 [8192, 128256], P(None, ('vocab', 'layer')), may hold values from -0.22097087 to 0.22097087
Outputs:
- log_probs: float32 [1024, 128256], P('layer', 'vocab')
The draws below stay inside these ranges and needn't reach their ends.
All inputs are finite; a program needn't handle non-finite values.
Results may differ from the reference program's by a relative error of at most 0.0003.
Values may be sent and summed in bfloat16 or wider, within the bound.
A program may use at most 192 MiB of HBM per device.

```python
import math
import jax
import jax.numpy as jnp
from jax import lax

D = 8192
VOCAB = 128256
TOK = 16
ROWS = 1024


def loud_offset(key):
    return jax.random.randint(jax.random.fold_in(key, 103), (), 0, 32)


def column_of(key, column):
    gaussian = jax.random.truncated_normal(jax.random.fold_in(jax.random.fold_in(key, 101), column), -4.0, 4.0, (D,), jnp.float32)
    spread = jax.random.uniform(jax.random.fold_in(jax.random.fold_in(key, 102), column), (), jnp.float32, -0.5, 0.5)
    loud = jnp.where(column % 32 == loud_offset(key), max(1.0, 80.0 / math.sqrt(D)), 1.0)
    return gaussian * (3.0 * jnp.exp(spread) * loud / math.sqrt(D))


def unit_column(key, column):
    vector = column_of(key, column)
    return vector / jnp.sqrt(jnp.mean(vector * vector))


def draw_unembed(key, part):
    columns = jax.vmap(lambda column: column_of(key, column))(jnp.arange(VOCAB))
    return columns.T.astype(jnp.bfloat16)


def draw_residual(key, part):
    offset = loud_offset(key)
    first = offset + 32 * jax.random.randint(jax.random.fold_in(key, 203), (ROWS,), 0, VOCAB // 32)
    second = offset + 32 * jax.random.randint(jax.random.fold_in(key, 204), (ROWS,), 0, VOCAB // 32)
    aligned = jax.vmap(lambda column: unit_column(key, column))(first)
    aligned = aligned + 0.99 * jax.vmap(lambda column: unit_column(key, column))(second)
    chosen = (jnp.arange(ROWS) % TOK == 0)[:, None]
    noise = jax.random.truncated_normal(jax.random.fold_in(key, 201), -4.0, 4.0, (ROWS, D), jnp.float32)
    scales = jnp.exp(jax.random.uniform(jax.random.fold_in(key, 202), (ROWS, 1), jnp.float32, 0.0, math.log(10.0)))
    strength = jnp.exp(jax.random.uniform(jax.random.fold_in(key, 205), (ROWS, 1), jnp.float32, math.log(0.2), math.log(2.0)))
    mixed = jnp.where(chosen, strength * (aligned + 0.1 * noise), noise * scales)
    return mixed.astype(jnp.bfloat16)


def setup_inputs(seed: int = 0) -> dict:
    key_of = jax.random.split(jax.random.key(seed), 4)
    residual = draw_residual(jax.random.fold_in(key_of[3], 71), 0)
    gain = jnp.clip(1.0 + 0.15 * jax.random.normal(key_of[1], (1, D), jnp.float32), 0.25, 1.75).astype(jnp.bfloat16)
    unembed = draw_unembed(jax.random.fold_in(key_of[3], 71), 0)
    return dict(residual=residual, gain=gain, unembed=unembed)


def reference(residual, gain, unembed):
    widened = residual.astype(jnp.float32)
    inverse = lax.rsqrt(lax.optimization_barrier(jnp.sum(widened * widened, axis=1)) / D + 1e-05)
    scaled = (widened * gain.astype(jnp.float32)).astype(jnp.bfloat16)
    logits = jnp.dot(scaled, unembed, preferred_element_type=jnp.float32) * inverse[:, None]
    highest = lax.optimization_barrier(jnp.max(logits, axis=1, keepdims=True))
    lse = highest + jnp.log(lax.optimization_barrier(jnp.sum(jnp.exp(logits - highest), axis=1, keepdims=True)))
    return logits - lse
```

```python
import jax
import jax.numpy as jnp
from jax import lax
from jax.sharding import PartitionSpec as P


def to_partner(value, step, size):
    return lax.ppermute(value, "layer", [(l, l ^ step) for l in range(size)])


def ring_of(size):
    return list(range(0, size, 2)) + list(range(1, size, 2))[::-1]


def ring_gather(block, place):
    size = lax.axis_size("vocab")
    ring = ring_of(size)
    order = jnp.array(ring, jnp.int32)
    where = jnp.array([ring.index(v) for v in range(size)], jnp.int32)[lax.axis_index("vocab")]
    up = [(ring[p], ring[(p + 1) % size]) for p in range(size)]
    down = [(b, a) for a, b in up]
    half, rows = size // 2, block.shape[0]
    place(block, order[where], 0)
    forward = backward = block
    for k in range(1, half + 1):
        if k == half and size % 2 == 0:
            forward, backward = forward[: rows // 2], backward[rows // 2 :]
        forward = lax.ppermute(forward, "vocab", up)
        backward = lax.ppermute(backward, "vocab", down)
        if k == max(half - 1, 1):
            nearly = (forward, backward)
        place(forward, order[(where - k) % size], 0)
        place(backward, order[(where + k) % size], rows - backward.shape[0])
    return nearly


def body(residual, gain, unembed):
    layers = lax.axis_size("layer")
    vocabs = lax.axis_size("vocab")
    rows, depth = residual.shape
    columns = unembed.shape[1]
    me = lax.axis_index("layer")
    width = depth * vocabs

    widened = residual.astype(jnp.float32)
    squares = jnp.sum(widened * widened, axis=1)
    scaled = (widened * gain.astype(jnp.float32)).astype(jnp.bfloat16)

    total = lax.all_gather(squares, "vocab").sum(0)
    own_inverse = lax.rsqrt(total / width + 1e-05)
    inverse = [to_partner(own_inverse, s, layers) if s else own_inverse for s in range(layers)]

    evens = [s for s in range(layers - 2, -1, -2)] if layers > 1 else [0]
    firsts = {s: to_partner(scaled, s, layers) if s else scaled for s in evens}
    full = {}
    after = own_inverse
    for step in evens:
        first, _ = lax.optimization_barrier((firsts[step], after))
        if step == 0:
            full[0] = lax.all_gather(first, "vocab", axis=1, tiled=True)
            break
        steps = [step, step + 1] if layers > 1 else [step]
        for s in steps:
            full[s] = jnp.zeros((rows, width), jnp.bfloat16)

        def place(block, owner, row):
            column = owner * depth
            full[step] = lax.dynamic_update_slice(full[step], block, (row, column))
            if layers > 1:
                other = to_partner(block, 1, layers)
                full[step + 1] = lax.dynamic_update_slice(full[step + 1], other, (row, column))

        after = ring_gather(first, place)

    order = [s for e in evens for s in ([e, e + 1] if layers > 1 else [e])]
    sent, heads = {}, {}
    for at, step in enumerate(order):
        inv = inverse[step]
        if step == 0 and layers > 1:
            full[1] = to_partner(full[0], 1, layers)
        products = lax.dot_general(
            unembed, full[step], (((0,), (1,)), ((), ())), preferred_element_type=jnp.float32
        )
        logits = products * inv[None, :]
        highest = jnp.max(logits, axis=0)
        centre = jnp.mean(logits, axis=0)
        totals = jnp.sum(jnp.exp(logits - highest[None, :]), axis=0)
        head = jnp.stack([highest, totals, centre])
        if step:
            heads[step] = to_partner(head, step, layers)
            short = (logits - centre[None, :]).astype(jnp.float16)
            if at + 1 < len(order) and order[at + 1] in full:
                following = order[at + 1]
                short, full[following] = lax.optimization_barrier((short, full[following]))
            sent[step] = to_partner(short, step, layers)
        else:
            heads[step] = head
            sent[step] = logits

    mine = jnp.stack([heads[s] for s in range(layers)])
    everyone = lax.all_gather(mine, "vocab")
    highest = jnp.max(everyone[:, :, 0], axis=(0, 1))
    totals = jnp.sum(everyone[:, :, 1] * jnp.exp(everyone[:, :, 0] - highest), axis=(0, 1))
    lse = highest + jnp.log(totals)

    out = jnp.zeros((layers, columns, rows), jnp.float32)
    for step in [0] + [s for s in order[::-1] if s]:
        if step:
            value = sent[step].astype(jnp.float32) + (mine[step, 2] - lse)[None, :]
        else:
            value = sent[step] - lse[None, :]
        out = lax.dynamic_update_slice(out, value[None], (me ^ step, 0, 0))
    return out.reshape(layers * columns, rows).T


def solution(mesh):
    placed = (P("layer", "vocab"), P(None, "vocab"), P(None, ("vocab", "layer")))
    return jax.shard_map(
        body, mesh=mesh, in_specs=placed, out_specs=P("layer", "vocab"), check_vma=False
    )
```
